32 devices in a mesh: depth: 8 (over z, x), rows: 4 (over y, core).
Axes of the slice: x: 2, y: 2, z: 4, core: 2. Of those that a mesh axis runs over, the one named last changes fastest.
Arguments:
- density: float32 [128, 64, 1024], P('depth', 'rows'), may hold values from 0 to 1
- bin_of_level: int32 [16], replicated, may hold values from 0 to 7
- absorb_bins: float32 [8], replicated, may hold values from 0.00234375 to 0.0625
- emit_bins: float32 [8], replicated, may hold values from 0.2 to 3
- occupancy: int32 [8, 4, 8], P('depth', 'rows'), may hold values 0 or 1
- col_offsets: int32 [1024], replicated, may hold values from 2 to 6
- row_offsets: int32 [64], P('rows'), may hold values from 2 to 6
Outputs:
- front_transmittance: float32 [8, 64, 1024], P('depth', 'rows')
- final_image: float32 [2, 64, 1024], P(None, 'rows')
The draws below stay inside these ranges and needn't reach their ends.
All inputs are finite; a program needn't handle non-finite values. No bound on the sum of `occupancy` on one device may be relied on, other than what follows from the above.
Results may differ from the reference program's by a relative error of at most 0.0002.
Values sent between devices are 32-bit elements; how exact they have to be, the bound alone decides.
No kernel may reach another device: no remote copies, remote signals or barrier semaphores. Data moves between devices by JAX's collectives and lax.ppermute only.
A program may use at most 64 MiB of HBM per device.

```python
import math
import jax
import jax.numpy as jnp
from jax import lax

COLS = 1024
LEVELS = 16
BINS = 8
SLAB = 16
ROW_DEV = 16
DEPTH_ALL = 128
ROWS_ALL = 64
TILES = 8
N_DEPTH = 8
N_ROWS = 4


def set_ends(entries, rng, smallest, top_value):
    place = [jax.random.randint(jax.random.fold_in(rng, axis), (), 0, length) for axis, length in enumerate(entries.shape)]
    widest = entries.shape.index(max(entries.shape))
    beside = place[:widest] + [(place[widest] + 1) % entries.shape[widest]] + place[widest + 1:]
    return entries.at[tuple(place)].set(smallest).at[tuple(beside)].set(top_value)


def block_scale(rng, shape, shards, least, largest):
    gain, own = 1.0, jax.random.fold_in(rng, 6)
    for axis_at, blocks in shards:
        heights = jnp.exp(jax.random.uniform(jax.random.fold_in(own, axis_at), (blocks,), jnp.float32, least / len(shards), largest / len(shards)))
        gain = gain * jnp.repeat(heights, shape[axis_at] // blocks).reshape([-1 if axis == axis_at else 1 for axis in range(len(shape))])
    return gain


def setup_inputs(seed: int = 0) -> dict:
    key_list = jax.random.split(jax.random.key(seed), 8)
    return {
        "density": jnp.clip(1.0 * jax.random.uniform(key_list[0], (DEPTH_ALL, ROWS_ALL, COLS), jnp.float32) ** block_scale(key_list[0], (DEPTH_ALL, ROWS_ALL, COLS), ((0, 8), (1, 4)), -0.2, 0.2), 0.0, 1.0),
        "bin_of_level": set_ends(jax.random.randint(key_list[1], (LEVELS,), 0, BINS), jax.random.fold_in(key_list[1], 1), 0, BINS - 1).astype(jnp.int32),
        "absorb_bins": jnp.clip(jnp.exp(jax.random.uniform(key_list[2], (BINS,), jnp.float32, math.log(0.00234375), math.log(0.0625))), 0.00234375, 0.0625),
        "emit_bins": jnp.clip(jnp.exp(jax.random.uniform(key_list[3], (BINS,), jnp.float32, math.log(0.2), math.log(3.0))), 0.2, 3.0),
        "occupancy": set_ends((jax.random.randint(key_list[4], (N_DEPTH, N_ROWS, TILES), 0, 4) < 3).astype(jnp.int32), jax.random.fold_in(key_list[4], 1), 0, 1),
        "col_offsets": set_ends(jax.random.randint(key_list[5], (COLS,), 2, 7), jax.random.fold_in(key_list[5], 1), 2, 6).astype(jnp.int32),
        "row_offsets": set_ends(jax.random.randint(key_list[6], (ROWS_ALL,), 2, 7), jax.random.fold_in(key_list[6], 1), 2, 6).astype(jnp.int32),
    }


def resample_columns(mixed, col_offsets):
    fraction = col_offsets.astype(jnp.float32) / 8.0
    pad_shape = mixed.shape[:-1] + (1,)
    right_side = jnp.concatenate([mixed[..., 1:], jnp.zeros(pad_shape, jnp.float32)], -1)
    return (1.0 - fraction) * mixed + fraction * right_side


def tables(bin_of_level, absorb_bins, emit_bins):
    count_bins = absorb_bins.shape[0]
    onehot = (bin_of_level[:, None] == jnp.arange(count_bins, dtype=jnp.int32)[None, :]).astype(jnp.float32)
    return jnp.sum(onehot * absorb_bins[None, :], 1), jnp.sum(onehot * emit_bins[None, :], 1)


def classify(sampled, absorb_level, emit_level):
    levels = absorb_level.shape[0]
    scaled = sampled * float(levels - 1)
    absorption = jnp.zeros(sampled.shape, jnp.float32)
    emission = jnp.zeros(sampled.shape, jnp.float32)
    for knot_index in range(levels):
        weight = jnp.maximum(0.0, 1.0 - jnp.abs(scaled - float(knot_index)))
        absorption = absorption + weight * absorb_level[knot_index]
        emission = emission + weight * emit_level[knot_index]
    return absorption, emission


def composite(absorption, emission):
    inclusive = jnp.cumsum(absorption, 0)
    exclusive = inclusive - absorption
    light = jnp.sum(jnp.exp(-exclusive) * (1.0 - jnp.exp(-absorption)) * emission, 0)
    return light, inclusive[-1]


def reference(density, bin_of_level, absorb_bins, emit_bins, occupancy, col_offsets, row_offsets):
    absorb_level, emit_level = tables(bin_of_level, absorb_bins, emit_bins)
    frac_row = (row_offsets.astype(jnp.float32) / 8.0)[None, :, None]
    slabs = density.reshape(N_DEPTH, SLAB, ROWS_ALL, COLS)
    followers = jnp.concatenate([slabs[1:, 0], jnp.zeros((1, ROWS_ALL, COLS), jnp.float32)], 0)

    def per_slab(inputs):
        planes, following, occupied = inputs
        extended = jnp.concatenate([planes, following[None]], 0)
        mid_depth = 0.5 * (extended[:-1] + extended[1:])
        next_rows = jnp.concatenate([mid_depth[:, 1:], jnp.zeros((SLAB, 1, COLS), jnp.float32)], 1)
        mixed = (1.0 - frac_row) * mid_depth + frac_row * next_rows
        sampled = resample_columns(mixed, col_offsets)
        absorption, emission = classify(sampled, absorb_level, emit_level)
        brick_mask = jnp.repeat(jnp.repeat(occupied.astype(jnp.float32), ROW_DEV, 0), 128, 1)
        absorption = absorption * brick_mask[None]
        return composite(absorption, emission)

    lights, depths = lax.map(per_slab, (slabs, followers, occupancy))
    front_depth = jnp.cumsum(depths, 0) - depths
    front = jnp.exp(-front_depth)
    radiance = jnp.sum(front * lights, 0)
    remaining = jnp.exp(-jnp.sum(depths, 0))
    return front, jnp.stack([radiance, remaining])
```

```python
import functools
import math

import jax
import jax.numpy as jnp
from jax import lax
from jax.experimental import pallas as pl
from jax.experimental.pallas import tpu as pltpu
from jax.sharding import PartitionSpec as P

WIDTH = 256


def from_behind(block, axis):
    size = lax.axis_size(axis)
    return lax.ppermute(block, axis, [(i + 1, i) for i in range(size - 1)])


def from_diagonal(block):
    depth, rows = lax.axis_size("depth"), lax.axis_size("rows")
    route = [
        ((z + 1) * rows + y + 1, z * rows + y)
        for z in range(depth - 1)
        for y in range(rows - 1)
    ]
    return lax.ppermute(block, ("depth", "rows"), route)


def tables(bin_of_level, absorb_bins, emit_bins):
    count_bins = absorb_bins.shape[0]
    onehot = bin_of_level[:, None] == jnp.arange(count_bins, dtype=jnp.int32)[None, :]

    def coefficients(bins):
        level = jnp.sum(jnp.where(onehot, bins[None, :], 0.0), 1)
        slope = level[1:] - level[:-1]
        gain = jnp.concatenate([slope[:1], slope[1:] - slope[:-1]])
        knots = jnp.arange(gain.shape[0], dtype=jnp.float32)
        base = level[0] - jnp.sum(gain * knots)
        rows = jnp.concatenate([base[None], gain])
        return jnp.broadcast_to(rows[:, None], (rows.shape[0], 128))

    return coefficients(absorb_bins * (-1.0 / math.log(2.0))), coefficients(emit_bins)


def render(density, plane, row, corner, weights, fraction, occupied, absorb, emit, state, scaled):
    planes, rows, cols = density.shape
    levels = absorb.shape[0]
    last_row = lax.broadcasted_iota(jnp.int32, (rows, 128), 0) == rows - 1
    last_lane = lax.broadcasted_iota(jnp.int32, (rows, 128), 1) == 127
    near, far = weights[0], weights[1]

    @pl.loop(0, planes)
    def _(z):
        last = z == planes - 1
        after = jnp.minimum(z + 1, planes - 1)

        def mixed(tile):
            at = pl.ds(tile * 128, 128)
            behind = jnp.where(last, plane[0, :, at], density[after, :, at])
            mid = density[z, :, at] + behind
            below = row[z, :, at] + jnp.where(last, corner[0, :, at], row[after, :, at])
            shifted = jnp.where(last_row, below, pltpu.roll(mid, rows - 1, 0))
            return near * mid + far * shifted

        current = mixed(0)
        rolled = pltpu.roll(current, 127, 1)
        tiles = cols // 128
        for tile in range(tiles):
            if tile + 1 < tiles:
                following = mixed(tile + 1)
                following_rolled = pltpu.roll(following, 127, 1)
                right = jnp.where(last_lane, following_rolled, rolled)
            else:
                right = jnp.where(last_lane, 0.0, rolled)
            part = fraction[tile : tile + 1, :]
            scaled[z, :, pl.ds(tile * 128, 128)] = (1.0 - part) * current + part * right
            if tile + 1 < tiles:
                current, rolled = following, following_rolled

    @pl.loop(0, cols // WIDTH)
    def _(tile):
        at = pl.ds(pl.multiple_of(tile * WIDTH, WIDTH), WIDTH)
        shape = (rows, WIDTH)
        mask = jnp.concatenate(
            [
                jnp.broadcast_to(occupied[pl.ds(tile * (WIDTH // 128) + i, 1), :], (rows, 128))
                for i in range(WIDTH // 128)
            ],
            1,
        )

        def splat(ref, k):
            return jnp.broadcast_to(jnp.concatenate([ref[k : k + 1, :]] * (WIDTH // 128), 1), shape)

        total = jnp.zeros(shape, jnp.float32)
        through = jnp.ones(shape, jnp.float32)
        light = jnp.zeros(shape, jnp.float32)
        for z in range(planes):
            value = scaled[z, :, at]
            absorption = splat(absorb, 0) + splat(absorb, 1) * value
            emission = splat(emit, 0) + splat(emit, 1) * value
            for k in range(1, levels - 1):
                kink = jnp.maximum(value, float(k))
                absorption += splat(absorb, k + 1) * kink
                emission += splat(emit, k + 1) * kink
            total += absorption * mask
            behind = jnp.exp2(total)
            light += (through - behind) * emission
            through = behind
        state[0, :, at] = light
        state[1, :, at] = through


def on_device(density, bin_of_level, absorb_bins, emit_bins, occupancy, col_offsets, row_offsets):
    planes, rows, cols = density.shape
    plane = from_behind(density[:1], "depth")
    row = from_behind(density[:, :1], "rows")
    corner = from_diagonal(density[:1, :1])
    absorb, emit = tables(bin_of_level, absorb_bins, emit_bins)
    levels = bin_of_level.shape[0]
    frac_row = row_offsets.astype(jnp.float32) / 8.0
    scale = 0.5 * (levels - 1)
    weights = jnp.broadcast_to(
        scale * jnp.stack([1.0 - frac_row, frac_row])[:, :, None], (2, rows, 128)
    )
    fraction = (col_offsets.astype(jnp.float32) / 8.0).reshape(cols // 128, 128)
    occupied = jnp.broadcast_to(
        occupancy[0, 0].astype(jnp.float32)[:, None], (cols // 128, 128)
    )
    vmem = pl.BlockSpec(memory_space=pltpu.VMEM)
    state = pl.pallas_call(
        render,
        out_shape=jax.ShapeDtypeStruct((2, rows, cols), jnp.float32),
        in_specs=[vmem] * 9,
        out_specs=vmem,
        scratch_shapes=[pltpu.VMEM((planes, rows, cols), jnp.float32)],
        cost_estimate=pl.CostEstimate(
            flops=100 * density.size, bytes_accessed=4 * density.size, transcendentals=density.size
        ),
        name="render",
    )(density, plane, row, corner, weights, fraction, occupied, absorb, emit)

    size = lax.axis_size("depth")
    position = lax.axis_index("depth")
    front = jnp.ones((1, rows, cols), jnp.float32)
    step = 1
    while step < size:
        other = lax.ppermute(state, "depth", [(i, i ^ step) for i in range(size)])
        behind = (position & step) != 0
        first = jnp.where(behind, other, state)
        second = jnp.where(behind, state, other)
        front = front * jnp.where(behind, other[1:], 1.0)
        state = jnp.stack([first[0] + first[1] * second[0], first[1] * second[1]])
        step *= 2
    return (front, state)


def solution(mesh):
    placed = (P("depth", "rows", None), P(), P(), P(), P("depth", "rows", None), P(), P("rows"))
    return jax.shard_map(
        on_device,
        mesh=mesh,
        in_specs=placed,
        out_specs=(P("depth", "rows", None), P(None, "rows", None)),
        check_vma=False,
    )
```

```python
import functools
import math

import jax
import jax.numpy as jnp
from jax import lax
from jax.experimental import pallas as pl
from jax.experimental.pallas import tpu as pltpu
from jax.sharding import PartitionSpec as P

SUB, LANES = 8, 128
F32 = jnp.float32
VMEM = pl.BlockSpec(memory_space=pltpu.VMEM)
SMEM = pl.BlockSpec(memory_space=pltpu.SMEM)
HBM = pl.BlockSpec(memory_space=pltpu.HBM)


def params(mib):
    return pltpu.CompilerParams(vmem_limit_bytes=mib << 20)


def from_behind(block, axis):
    size = lax.axis_size(axis)
    return lax.ppermute(block, axis, [(i + 1, i) for i in range(size - 1)])


def from_diagonal(block):
    depth, rows = lax.axis_size("depth"), lax.axis_size("rows")
    route = [
        ((z + 1) * rows + y + 1, z * rows + y)
        for z in range(depth - 1)
        for y in range(rows - 1)
    ]
    return lax.ppermute(block, ("depth", "rows"), route)


def wide(row):
    return jnp.broadcast_to(row, (SUB, LANES))


def edges_kernel(density, plane, row, corner, last_row, sems):
    height = density.shape[1]
    pieces = [
        (density.at[0, 0, :, 0, :], corner),
        (density.at[:, 0, :, 0, :], row),
        (density.at[0], plane),
        (density.at[:, height - 1, :, SUB - 1, :], last_row),
    ]
    copies = [pltpu.make_async_copy(a, b, sems.at[i]) for i, (a, b) in enumerate(pieces)]
    for copy in copies:
        copy.start()
    for copy in copies:
        copy.wait()


def hats(values, table, levels):
    def at(k):
        return wide(table[k : k + 1, :])

    absorption = [at(0) + at(1) * u for u in values]
    emission = [at(levels) + at(levels + 1) * u for u in values]
    for k in range(1, levels - 1):
        gain_a, gain_e = at(k + 1), at(levels + k + 1)
        for j, u in enumerate(values):
            kink = jnp.maximum(u, float(k))
            absorption[j] = absorption[j] + gain_a * kink
            emission[j] = emission[j] + gain_e * kink
    return absorption, emission


def interior_kernel(
    bins, absorb_bins, emit_bins, occupied, row_offsets, col_offsets, density,
    state, table, columns, rows, weights, scaled,
):
    planes, height, tiles = density.shape[:3]
    levels = bins.shape[0]
    for first, level, unit in ((0, absorb_bins, -1.0 / math.log(2.0)), (levels, emit_bins, 1.0)):
        value = [level[bins[k]] * unit for k in range(levels)]
        base, before = value[0], 0.0
        for k in range(levels - 1):
            slope = value[k + 1] - value[k]
            gain = slope - before
            before = slope
            base = base - gain * float(k)
            table[first + k + 1 : first + k + 2, :] = jnp.full((1, LANES), gain, F32)
        table[first : first + 1, :] = jnp.full((1, LANES), base, F32)

    sub = lax.broadcasted_iota(jnp.int32, (SUB, LANES), 0)
    lane_end = lax.broadcasted_iota(jnp.int32, (SUB, LANES), 1) == LANES - 1
    row_end = sub == SUB - 1
    scale = 0.5 * (levels - 1)
    near, far = [], []
    for r in range(height):
        offset = jnp.zeros((SUB, LANES), F32)
        for i in range(SUB):
            step = row_offsets[r * SUB + i].astype(F32) * (scale / 8.0)
            offset = jnp.where(sub == i, step, offset)
        far.append(offset)
        near.append(scale - offset)
        weights[0, r] = near[r]
        weights[1, r] = far[r]
    rows[0:1, :] = near[-1][SUB - 1 :, :]
    rows[1:2, :] = far[-1][SUB - 1 :, :]

    shape = (tiles, LANES)
    fraction = col_offsets[...].astype(F32) * 0.125
    ends = (lax.broadcasted_iota(jnp.int32, shape, 0) == tiles - 1) & (
        lax.broadcasted_iota(jnp.int32, shape, 1) == LANES - 1
    )
    columns[0] = 1.0 - fraction
    columns[1] = jnp.where(ends, 0.0, fraction)
    for t in range(tiles):
        columns[2, t : t + 1, :] = jnp.full((1, LANES), occupied[t].astype(F32), F32)

    for z in range(planes - 1):

        def mixed(t):
            mid = [density[z, r, t] + density[z + 1, r, t] for r in range(height)]
            up = [pltpu.roll(m, SUB - 1, 0) for m in mid]
            below = [
                jnp.where(row_end, up[r + 1], up[r]) if r + 1 < height else up[r]
                for r in range(height)
            ]
            return [near[r] * mid[r] + far[r] * below[r] for r in range(height)]

        now = mixed(0)
        turned = [pltpu.roll(m, LANES - 1, 1) for m in now]
        for t in range(tiles):
            if t + 1 < tiles:
                after = mixed(t + 1)
                after_turned = [pltpu.roll(m, LANES - 1, 1) for m in after]
            else:
                after, after_turned = now, turned
            left, right = columns[0, t : t + 1, :], columns[1, t : t + 1, :]
            for r in range(height):
                beside = jnp.where(lane_end, after_turned[r], turned[r])
                scaled[z, r, t] = left * now[r] + right * beside
            now, turned = after, after_turned

    @pl.loop(0, tiles)
    def _(t):
        mask = wide(columns[2, pl.ds(t, 1), :])
        total = [jnp.zeros((SUB, LANES), F32)] * height
        through = [jnp.ones((SUB, LANES), F32)] * height
        light = [jnp.zeros((SUB, LANES), F32)] * height
        for z in range(planes - 1):
            absorption, emission = hats([scaled[z, r, t] for r in range(height)], table, levels)
            for r in range(height):
                total[r] = total[r] + absorption[r] * mask
                behind = jnp.exp2(total[r])
                light[r] = light[r] + (through[r] - behind) * emission[r]
                through[r] = behind
        for r in range(height):
            state[0, r, t] = light[r]
            state[1, r, t] = through[r]


def boundary_kernel(
    density, plane, row, corner, last_row, table, columns, rows, weights, before, state, *, levels
):
    planes, height, tiles = density.shape[:3]
    lane_end = lax.broadcasted_iota(jnp.int32, (SUB, LANES), 1) == LANES - 1
    row_end = lax.broadcasted_iota(jnp.int32, (SUB, LANES), 0) == SUB - 1

    mid = [[density[planes - 1, r, t] + plane[r, t] for t in range(tiles)] for r in range(height)]
    up = [[pltpu.roll(m, SUB - 1, 0) for m in line] for line in mid]
    value = []
    for r in range(height):
        line = []
        for t in range(tiles):
            below = jnp.where(row_end, up[r + 1][t], up[r][t]) if r + 1 < height else up[r][t]
            line.append(weights[0, r] * mid[r][t] + weights[1, r] * below)
        turned = [pltpu.roll(m, LANES - 1, 1) for m in line]
        for t in range(tiles):
            beside = jnp.where(lane_end, turned[min(t + 1, tiles - 1)], turned[t])
            value.append(columns[0, t : t + 1, :] * line[t] + columns[1, t : t + 1, :] * beside)
    group = 4
    for first in range(0, height * tiles, group):
        where = [divmod(j, tiles) for j in range(first, min(first + group, height * tiles))]
        absorption, emission = hats(value[first : first + group], table, levels)
        for (r, t), a, e in zip(where, absorption, emission, strict=True):
            through = before[1, r, t]
            behind = through * jnp.exp2(a * wide(columns[2, t : t + 1, :]))
            state[0, r, t] = before[0, r, t] + (through - behind) * e
            state[1, r, t] = behind

    shape = (tiles, LANES)
    fold_end = lax.broadcasted_iota(jnp.int32, shape, 1) == LANES - 1
    near, far = rows[0:1, :], rows[1:2, :]
    left, right = columns[0], columns[1]
    last_plane = jnp.concatenate([plane[height - 1, t, SUB - 1 :, :] for t in range(tiles)], 0)
    own = [last_row[z] for z in range(planes)] + [last_plane]
    under = [row[z] for z in range(planes)] + [corner[...]]
    value = []
    for z in range(planes):
        line = near * (own[z] + own[z + 1]) + far * (under[z] + under[z + 1])
        turned = pltpu.roll(line, LANES - 1, 1)
        beside = jnp.where(fold_end, pltpu.roll(turned, tiles - 1, 0), turned)
        value.append(left * line + right * beside)
    total = jnp.zeros(shape, F32)
    through = jnp.ones(shape, F32)
    light = jnp.zeros(shape, F32)
    for first in range(0, planes, group):
        absorption, emission = hats(value[first : first + group], table, levels)
        for a, e in zip(absorption, emission, strict=True):
            total = total + a * columns[2]
            behind = jnp.exp2(total)
            light = light + (through - behind) * e
            through = behind
    for t in range(tiles):
        state[0, height - 1, t, SUB - 1 :, :] = light[t : t + 1, :]
        state[1, height - 1, t, SUB - 1 :, :] = through[t : t + 1, :]


def merge(state, other, front, step):
    behind = (lax.axis_index("depth") & step) != 0
    first = jnp.where(behind, other, state)
    second = jnp.where(behind, state, other)
    front = front * jnp.where(behind, other[1:], 1.0)
    return jnp.stack([first[0] + first[1] * second[0], first[1] * second[1]]), front


def on_device(density, bin_of_level, absorb_bins, emit_bins, occupancy, col_offsets, row_offsets):
    planes, rows, cols = density.shape
    height, tiles = rows // SUB, cols // LANES
    levels = bin_of_level.shape[0]
    tiled = density.reshape(planes, height, SUB, tiles, LANES).transpose(0, 1, 3, 2, 4)
    flat = (height, tiles, SUB, LANES)

    def out(*shape):
        return jax.ShapeDtypeStruct(shape, F32)

    plane, row, corner, last_row = pl.pallas_call(
        edges_kernel,
        out_shape=[
            out(*flat), out(planes, tiles, LANES), out(tiles, LANES), out(planes, tiles, LANES)
        ],
        in_specs=[HBM],
        out_specs=[VMEM] * 4,
        scratch_shapes=[pltpu.SemaphoreType.DMA((4,))],
        compiler_params=params(2),
        name="edges",
    )(tiled)
    row = from_behind(row, "rows")
    plane = from_behind(plane, "depth")
    corner = from_diagonal(corner)

    work = density.size
    state, table, columns, last_weights, row_weights = pl.pallas_call(
        interior_kernel,
        out_shape=[
            out(2, *flat), out(2 * levels, LANES), out(3, tiles, LANES), out(2, LANES),
            out(2, height, SUB, LANES),
        ],
        in_specs=[SMEM] * 5 + [VMEM] * 2,
        out_specs=[VMEM] * 5,
        scratch_shapes=[pltpu.VMEM((planes - 1, *flat), F32)],
        cost_estimate=pl.CostEstimate(
            flops=100 * work, bytes_accessed=4 * work, transcendentals=work
        ),
        compiler_params=params(8),
        name="interior",
    )(
        bin_of_level, absorb_bins, emit_bins, occupancy.reshape(tiles), row_offsets,
        col_offsets.reshape(tiles, LANES), tiled,
    )
    state = pl.pallas_call(
        functools.partial(boundary_kernel, levels=levels),
        out_shape=out(2, *flat),
        in_specs=[VMEM] * 10,
        out_specs=VMEM,
        compiler_params=params(8),
        name="boundary",
    )(tiled, plane, row, corner, last_row, table, columns, last_weights, row_weights, state)

    size = lax.axis_size("depth")
    front = jnp.ones((1, *flat), F32)
    step = 1
    while step < size:
        flip = step | (step >> 1) if 2 * step == size else step
        other = lax.ppermute(state, "depth", [(i, i ^ flip) for i in range(size)])
        state, front = merge(state, other, front, step)
        step *= 2

    def plain(block):
        return block.transpose(0, 1, 3, 2, 4).reshape(-1, rows, cols)

    return (plain(front), plain(state))


def solution(mesh):
    placed = (P("depth", "rows", None), P(), P(), P(), P("depth", "rows", None), P(), P("rows"))
    return jax.shard_map(
        on_device,
        mesh=mesh,
        in_specs=placed,
        out_specs=(P("depth", "rows", None), P(None, "rows", None)),
        check_vma=False,
    )
```

```python
import functools
import math

import jax
import jax.numpy as jnp
from jax import lax
from jax.experimental import pallas as pl
from jax.experimental.pallas import tpu as pltpu
from jax.sharding import PartitionSpec as P

SUB, LANES = 8, 128
F32 = jnp.float32
VMEM = pl.BlockSpec(memory_space=pltpu.VMEM)
SMEM = pl.BlockSpec(memory_space=pltpu.SMEM)
HBM = pl.BlockSpec(memory_space=pltpu.HBM)


def params(mib):
    return pltpu.CompilerParams(vmem_limit_bytes=mib << 20)


def from_behind(block, axis):
    size = lax.axis_size(axis)
    return lax.ppermute(block, axis, [(i + 1, i) for i in range(size - 1)])


def from_diagonal(block):
    depth, rows = lax.axis_size("depth"), lax.axis_size("rows")
    route = [
        ((z + 1) * rows + y + 1, z * rows + y)
        for z in range(depth - 1)
        for y in range(rows - 1)
    ]
    return lax.ppermute(block, ("depth", "rows"), route)


def wide(row):
    return jnp.broadcast_to(row, (SUB, LANES))


def edges_kernel(
    density, bins, absorb_bins, emit_bins, occupied, row_offsets, col_offsets,
    plane, row, corner, last_row, small, columns, sems,
):
    height = density.shape[1]
    pieces = [
        (density.at[0, 0, :, 0, :], corner),
        (density.at[:, 0, :, 0, :], row),
        (density.at[0], plane),
        (density.at[:, height - 1, :, SUB - 1, :], last_row),
    ]
    copies = [pltpu.make_async_copy(a, b, sems.at[i]) for i, (a, b) in enumerate(pieces)]
    for copy in copies:
        copy.start()
    small[...] = jnp.zeros_like(small)
    for i, source in enumerate((bins, absorb_bins, emit_bins, occupied, row_offsets)):
        small[i : i + 1, : source.shape[1]] = source[...].astype(F32)
    fraction = col_offsets[...].astype(F32) * 0.125
    shape = fraction.shape
    ends = (lax.broadcasted_iota(jnp.int32, shape, 0) == shape[0] - 1) & (
        lax.broadcasted_iota(jnp.int32, shape, 1) == LANES - 1
    )
    columns[0] = 1.0 - fraction
    columns[1] = jnp.where(ends, 0.0, fraction)
    for copy in copies:
        copy.wait()


def hats(values, table, levels):
    def at(k):
        return wide(table[k : k + 1, :])

    absorption = [at(0) + at(1) * u for u in values]
    emission = [at(levels) + at(levels + 1) * u for u in values]
    for k in range(1, levels - 1):
        gain_a, gain_e = at(k + 1), at(levels + k + 1)
        for j, u in enumerate(values):
            kink = jnp.maximum(u, float(k))
            absorption[j] = absorption[j] + gain_a * kink
            emission[j] = emission[j] + gain_e * kink
    return absorption, emission


def interior_kernel(small, columns, density, state, table, masks, rows, weights, scaled, *, levels):
    planes, height, tiles = density.shape[:3]
    lane = lax.broadcasted_iota(jnp.int32, (SUB, LANES), 1)
    sub = lax.broadcasted_iota(jnp.int32, (SUB, LANES), 0)
    lane_end, row_end = lane == LANES - 1, sub == SUB - 1
    bins, absorb_bins, emit_bins, occupied, row_offsets = (
        wide(small[i : i + 1, :]) for i in range(5)
    )

    def pick(vector, k):
        return jnp.broadcast_to(vector[:, k : k + 1], (SUB, LANES))

    scale = 0.5 * (levels - 1)
    near, far = [], []
    for r in range(height):
        offset = jnp.zeros((SUB, LANES), F32)
        for i in range(SUB):
            offset = jnp.where(sub == i, pick(row_offsets, r * SUB + i), offset)
        far.append(offset * (scale / 8.0))
        near.append(scale - far[r])
        weights[0, r] = near[r]
        weights[1, r] = far[r]
    rows[0:1, :] = near[-1][SUB - 1 :, :]
    rows[1:2, :] = far[-1][SUB - 1 :, :]
    for t in range(tiles):
        masks[t : t + 1, :] = pick(occupied, t)[:1, :]

    which = bins.astype(jnp.int32)
    for first, level, unit in ((0, absorb_bins, -1.0 / math.log(2.0)), (levels, emit_bins, 1.0)):
        value = jnp.take_along_axis(level, which, axis=1, mode="promise_in_bounds") * unit
        slope = pltpu.roll(value, LANES - 1, 1) - value
        gain = jnp.where(lane == 0, slope, slope - pltpu.roll(slope, 1, 1))
        shift = jnp.where(lane < levels - 1, gain * lane.astype(F32), 0.0)
        base = pick(value, 0) - jnp.sum(shift, 1, keepdims=True)
        table[first : first + 1, :] = base[:1, :]
        for k in range(levels - 1):
            table[first + k + 1 : first + k + 2, :] = pick(gain, k)[:1, :]

    for z in range(planes - 1):

        def mixed(t):
            mid = [density[z, r, t] + density[z + 1, r, t] for r in range(height)]
            up = [pltpu.roll(m, SUB - 1, 0) for m in mid]
            below = [
                jnp.where(row_end, up[r + 1], up[r]) if r + 1 < height else up[r]
                for r in range(height)
            ]
            return [near[r] * mid[r] + far[r] * below[r] for r in range(height)]

        now = mixed(0)
        turned = [pltpu.roll(m, LANES - 1, 1) for m in now]
        for t in range(tiles):
            if t + 1 < tiles:
                after = mixed(t + 1)
                after_turned = [pltpu.roll(m, LANES - 1, 1) for m in after]
            else:
                after, after_turned = now, turned
            left, right = columns[0, t : t + 1, :], columns[1, t : t + 1, :]
            for r in range(height):
                beside = jnp.where(lane_end, after_turned[r], turned[r])
                scaled[z, r, t] = left * now[r] + right * beside
            now, turned = after, after_turned

    @pl.loop(0, tiles)
    def _(t):
        mask = wide(masks[pl.ds(t, 1), :])
        total = [jnp.zeros((SUB, LANES), F32)] * height
        through = [jnp.ones((SUB, LANES), F32)] * height
        light = [jnp.zeros((SUB, LANES), F32)] * height
        for z in range(planes - 1):
            absorption, emission = hats([scaled[z, r, t] for r in range(height)], table, levels)
            for r in range(height):
                total[r] = total[r] + absorption[r] * mask
                behind = jnp.exp2(total[r])
                light[r] = light[r] + (through[r] - behind) * emission[r]
                through[r] = behind
        for r in range(height):
            state[0, r, t] = light[r]
            state[1, r, t] = through[r]


def boundary_kernel(
    density, plane, row, corner, last_row, table, columns, masks, rows, weights, before, state, *, levels
):
    planes, height, tiles = density.shape[:3]
    lane_end = lax.broadcasted_iota(jnp.int32, (SUB, LANES), 1) == LANES - 1
    row_end = lax.broadcasted_iota(jnp.int32, (SUB, LANES), 0) == SUB - 1

    mid = [[density[planes - 1, r, t] + plane[r, t] for t in range(tiles)] for r in range(height)]
    up = [[pltpu.roll(m, SUB - 1, 0) for m in line] for line in mid]
    value = []
    for r in range(height):
        line = []
        for t in range(tiles):
            below = jnp.where(row_end, up[r + 1][t], up[r][t]) if r + 1 < height else up[r][t]
            line.append(weights[0, r] * mid[r][t] + weights[1, r] * below)
        turned = [pltpu.roll(m, LANES - 1, 1) for m in line]
        for t in range(tiles):
            beside = jnp.where(lane_end, turned[min(t + 1, tiles - 1)], turned[t])
            value.append(columns[0, t : t + 1, :] * line[t] + columns[1, t : t + 1, :] * beside)
    group = 4
    for first in range(0, height * tiles, group):
        where = [divmod(j, tiles) for j in range(first, min(first + group, height * tiles))]
        absorption, emission = hats(value[first : first + group], table, levels)
        for (r, t), a, e in zip(where, absorption, emission, strict=True):
            through = before[1, r, t]
            behind = through * jnp.exp2(a * wide(masks[t : t + 1, :]))
            state[0, r, t] = before[0, r, t] + (through - behind) * e
            state[1, r, t] = behind

    shape = (tiles, LANES)
    fold_end = lax.broadcasted_iota(jnp.int32, shape, 1) == LANES - 1
    near, far = rows[0:1, :], rows[1:2, :]
    left, right = columns[0], columns[1]
    last_plane = jnp.concatenate([plane[height - 1, t, SUB - 1 :, :] for t in range(tiles)], 0)
    own = [last_row[z] for z in range(planes)] + [last_plane]
    under = [row[z] for z in range(planes)] + [corner[...]]
    value = []
    for z in range(planes):
        line = near * (own[z] + own[z + 1]) + far * (under[z] + under[z + 1])
        turned = pltpu.roll(line, LANES - 1, 1)
        beside = jnp.where(fold_end, pltpu.roll(turned, tiles - 1, 0), turned)
        value.append(left * line + right * beside)
    total = jnp.zeros(shape, F32)
    through = jnp.ones(shape, F32)
    light = jnp.zeros(shape, F32)
    for first in range(0, planes, group):
        absorption, emission = hats(value[first : first + group], table, levels)
        for a, e in zip(absorption, emission, strict=True):
            total = total + a * masks[...]
            behind = jnp.exp2(total)
            light = light + (through - behind) * e
            through = behind
    for t in range(tiles):
        state[0, height - 1, t, SUB - 1 :, :] = light[t : t + 1, :]
        state[1, height - 1, t, SUB - 1 :, :] = through[t : t + 1, :]


def is_behind(step):
    return (lax.axis_index("depth") & step) != 0


def merge(state, other, front, step):
    behind = is_behind(step)
    first = jnp.where(behind, other, state)
    second = jnp.where(behind, state, other)
    front = front * jnp.where(behind, other[1:], 1.0)
    return jnp.stack([first[0] + first[1] * second[0], first[1] * second[1]]), front


def last_merge_kernel(state, other, front, front_out, image_out, front_buf, image_buf, sems, *, step):
    behind = is_behind(step)
    light, through = state[0], state[1]
    other_light, other_through = other[0], other[1]
    front_buf[0] = front[0] * jnp.where(behind, other_through, 1.0)
    copy_front = pltpu.make_async_copy(front_buf, front_out, sems.at[0])
    copy_front.start()
    image_buf[0] = jnp.where(
        behind, other_light + other_through * light, light + through * other_light
    )
    image_buf[1] = through * other_through
    copy_image = pltpu.make_async_copy(image_buf, image_out, sems.at[1])
    copy_image.start()
    copy_front.wait()
    copy_image.wait()


def on_device(density, bin_of_level, absorb_bins, emit_bins, occupancy, col_offsets, row_offsets):
    planes, rows, cols = density.shape
    height, tiles = rows // SUB, cols // LANES
    levels = bin_of_level.shape[0]
    tiled = density.reshape(planes, height, SUB, tiles, LANES).transpose(0, 1, 3, 2, 4)
    flat = (height, tiles, SUB, LANES)

    def out(*shape):
        return jax.ShapeDtypeStruct(shape, F32)

    plane, row, corner, last_row, small, columns = pl.pallas_call(
        edges_kernel,
        out_shape=[
            out(*flat), out(planes, tiles, LANES), out(tiles, LANES), out(planes, tiles, LANES),
            out(SUB, LANES), out(2, tiles, LANES),
        ],
        in_specs=[HBM] + [VMEM] * 6,
        out_specs=[VMEM] * 6,
        scratch_shapes=[pltpu.SemaphoreType.DMA((4,))],
        compiler_params=params(2),
        name="edges",
    )(
        tiled, bin_of_level[None], absorb_bins[None], emit_bins[None],
        occupancy.reshape(1, tiles), row_offsets[None], col_offsets.reshape(tiles, LANES),
    )
    row = from_behind(row, "rows")
    plane = from_behind(plane, "depth")
    corner = from_diagonal(corner)

    work = density.size
    state, table, masks, last_weights, row_weights = pl.pallas_call(
        functools.partial(interior_kernel, levels=levels),
        out_shape=[
            out(2, *flat), out(2 * levels, LANES), out(tiles, LANES), out(2, LANES),
            out(2, height, SUB, LANES),
        ],
        in_specs=[VMEM] * 3,
        out_specs=[VMEM] * 5,
        scratch_shapes=[pltpu.VMEM((planes - 1, *flat), F32)],
        cost_estimate=pl.CostEstimate(
            flops=100 * work, bytes_accessed=4 * work, transcendentals=work
        ),
        compiler_params=params(8),
        name="interior",
    )(small, columns, tiled)
    state = pl.pallas_call(
        functools.partial(boundary_kernel, levels=levels),
        out_shape=out(2, *flat),
        in_specs=[VMEM] * 11,
        out_specs=VMEM,
        compiler_params=params(8),
        name="boundary",
    )(tiled, plane, row, corner, last_row, table, columns, masks, last_weights, row_weights, state)

    size = lax.axis_size("depth")
    front = jnp.ones((1, *flat), F32)
    step = 1
    while 2 * step < size:
        other = lax.ppermute(state, "depth", [(i, i ^ step) for i in range(size)])
        state, front = merge(state, other, front, step)
        step *= 2
    flip = step | (step >> 1)
    other = lax.ppermute(state, "depth", [(i, i ^ flip) for i in range(size)])
    front, state = pl.pallas_call(
        functools.partial(last_merge_kernel, step=step),
        out_shape=[out(1, *flat), out(2, *flat)],
        in_specs=[VMEM] * 3,
        out_specs=[HBM] * 2,
        scratch_shapes=[
            pltpu.VMEM((1, *flat), F32), pltpu.VMEM((2, *flat), F32), pltpu.SemaphoreType.DMA((2,))
        ],
        compiler_params=params(4),
        name="last_merge",
    )(state, other, front)

    def plain(block):
        return block.transpose(0, 1, 3, 2, 4).reshape(-1, rows, cols)

    return (plain(front), plain(state))


def solution(mesh):
    placed = (P("depth", "rows", None), P(), P(), P(), P("depth", "rows", None), P(), P("rows"))
    return jax.shard_map(
        on_device,
        mesh=mesh,
        in_specs=placed,
        out_specs=(P("depth", "rows", None), P(None, "rows", None)),
        check_vma=False,
    )
```

```python
import functools
import math

import jax
import jax.numpy as jnp
from jax import lax
from jax.experimental import pallas as pl
from jax.experimental.pallas import tpu as pltpu
from jax.sharding import PartitionSpec as P

SUB, LANES = 8, 128
F32 = jnp.float32
VMEM = pl.BlockSpec(memory_space=pltpu.VMEM)
HBM = pl.BlockSpec(memory_space=pltpu.HBM)
EDGES_VMEM = 67_043_328 - (512 << 10)


def params(mib):
    return pltpu.CompilerParams(vmem_limit_bytes=mib << 20)


def from_behind(block, axis):
    size = lax.axis_size(axis)
    return lax.ppermute(block, axis, [((i + 1) % size, i) for i in range(size)])


def plane_from_behind(plane):
    depth, rows = lax.axis_size("depth"), lax.axis_size("rows")
    even = lax.ppermute(plane, "depth", [(i, i ^ 1) for i in range(depth)])
    route = []
    for d in range(depth):
        for r in range(rows):
            end = d in (0, depth - 1)
            e, q = (d, r ^ 1) if end else ((d + 1 if d % 2 else d - 1), r)
            route.append((e * rows + q, d * rows + r))
    odd = lax.ppermute(plane, ("depth", "rows"), route)
    return jnp.where(lax.axis_index("depth") % 2 == 0, even, odd)


def unless_last(axis):
    return jnp.where(lax.axis_index(axis) == lax.axis_size(axis) - 1, 0.0, 1.0)


def wide(row):
    return jnp.broadcast_to(row, (SUB, LANES))


def edges_kernel(density, *refs):
    small, (plane, row, last_row, *small_out), sems = refs[:6], refs[6:15], refs[15]
    height = density.shape[1]
    pieces = [
        (density.at[0], plane),
        (density.at[:, 0, :, 0, :], row),
        (density.at[:, height - 1, :, SUB - 1, :], last_row),
        *zip(small, small_out, strict=True),
    ]
    copies = [pltpu.make_async_copy(a, b, sems.at[i]) for i, (a, b) in enumerate(pieces)]
    for copy in copies:
        copy.start()
    for copy in copies:
        copy.wait()


def hats(values, table, levels):
    def at(k):
        return wide(table[k : k + 1, :])

    absorption = [at(0) + at(1) * u for u in values]
    emission = [at(levels) + at(levels + 1) * u for u in values]
    for k in range(1, levels - 1):
        gain_a, gain_e = at(k + 1), at(levels + k + 1)
        for j, u in enumerate(values):
            kink = jnp.maximum(u, float(k))
            absorption[j] = absorption[j] + gain_a * kink
            emission[j] = emission[j] + gain_e * kink
    return absorption, emission


def interior_kernel(
    bins, absorb_bins, emit_bins, occupied, row_offsets, col_offsets, density,
    state, last_state, table, masks, columns, rows, weights, scaled, small,
):
    planes, height, tiles = density.shape[:3]
    levels = bins.shape[1]
    small[...] = jnp.zeros_like(small)
    for i, source in enumerate((bins, absorb_bins, emit_bins, occupied, row_offsets)):
        small[i : i + 1, : source.shape[1]] = source[...].astype(F32)
    fraction = col_offsets[...].astype(F32) * 0.125
    shape = fraction.shape
    ends = (lax.broadcasted_iota(jnp.int32, shape, 0) == tiles - 1) & (
        lax.broadcasted_iota(jnp.int32, shape, 1) == LANES - 1
    )
    columns[0] = 1.0 - fraction
    columns[1] = jnp.where(ends, 0.0, fraction)
    lane = lax.broadcasted_iota(jnp.int32, (SUB, LANES), 1)
    sub = lax.broadcasted_iota(jnp.int32, (SUB, LANES), 0)
    lane_end, row_end = lane == LANES - 1, sub == SUB - 1
    bins, absorb_bins, emit_bins, occupied, row_offsets = (
        wide(small[i : i + 1, :]) for i in range(5)
    )

    def pick(vector, k):
        return jnp.broadcast_to(vector[:, k : k + 1], (SUB, LANES))

    scale = 0.5 * (levels - 1)
    near, far = [], []
    for r in range(height):
        offset = jnp.zeros((SUB, LANES), F32)
        for i in range(SUB):
            offset = jnp.where(sub == i, pick(row_offsets, r * SUB + i), offset)
        far.append(offset * (scale / 8.0))
        near.append(scale - far[r])
        weights[0, r] = near[r]
        weights[1, r] = far[r]
    rows[0:1, :] = near[-1][SUB - 1 :, :]
    rows[1:2, :] = far[-1][SUB - 1 :, :]
    for t in range(tiles):
        masks[t : t + 1, :] = pick(occupied, t)[:1, :]

    which = bins.astype(jnp.int32)
    for first, level, unit in ((0, absorb_bins, -1.0 / math.log(2.0)), (levels, emit_bins, 1.0)):
        value = jnp.take_along_axis(level, which, axis=1, mode="promise_in_bounds") * unit
        slope = pltpu.roll(value, LANES - 1, 1) - value
        gain = jnp.where(lane == 0, slope, slope - pltpu.roll(slope, 1, 1))
        shift = jnp.where(lane < levels - 1, gain * lane.astype(F32), 0.0)
        base = pick(value, 0) - jnp.sum(shift, 1, keepdims=True)
        table[first : first + 1, :] = base[:1, :]
        for k in range(levels - 1):
            table[first + k + 1 : first + k + 2, :] = pick(gain, k)[:1, :]

    for z in range(planes - 1):

        def mixed(t):
            mid = [density[z, r, t] + density[z + 1, r, t] for r in range(height)]
            up = [pltpu.roll(m, SUB - 1, 0) for m in mid]
            below = [
                jnp.where(row_end, up[r + 1], up[r]) if r + 1 < height else up[r]
                for r in range(height)
            ]
            return [near[r] * mid[r] + far[r] * below[r] for r in range(height)]

        now = mixed(0)
        turned = [pltpu.roll(m, LANES - 1, 1) for m in now]
        for t in range(tiles):
            if t + 1 < tiles:
                after = mixed(t + 1)
                after_turned = [pltpu.roll(m, LANES - 1, 1) for m in after]
            else:
                after, after_turned = now, turned
            left, right = columns[0, t : t + 1, :], columns[1, t : t + 1, :]
            for r in range(height):
                beside = jnp.where(lane_end, after_turned[r], turned[r])
                scaled[z, r, t] = left * now[r] + right * beside
            now, turned = after, after_turned

    @pl.loop(0, tiles)
    def _(t):
        mask = wide(masks[pl.ds(t, 1), :])
        total = [jnp.zeros((SUB, LANES), F32)] * height
        through = [jnp.ones((SUB, LANES), F32)] * height
        light = [jnp.zeros((SUB, LANES), F32)] * height
        for z in range(planes - 1):
            absorption, emission = hats([scaled[z, r, t] for r in range(height)], table, levels)
            for r in range(height):
                total[r] = total[r] + absorption[r] * mask
                behind = jnp.exp2(total[r])
                light[r] = light[r] + (through[r] - behind) * emission[r]
                through[r] = behind
        for r in range(height - 1):
            state[0, r, t] = light[r]
            state[1, r, t] = through[r]
        last_state[0, 0, t] = light[-1]
        last_state[1, 0, t] = through[-1]


def add_last_plane(density, plane, table, masks, columns, weights, before, state, tiles_of_rows):
    planes, height, tiles = density.shape[:3]
    levels = table.shape[0] // 2
    some = unless_last("depth")
    lane_end = lax.broadcasted_iota(jnp.int32, (SUB, LANES), 1) == LANES - 1
    row_end = lax.broadcasted_iota(jnp.int32, (SUB, LANES), 0) == SUB - 1
    value = []
    for r in tiles_of_rows:
        line = []
        for t in range(tiles):
            mid = density[planes - 1, r, t] + some * plane[r, t]
            below = pltpu.roll(mid, SUB - 1, 0)
            if r + 1 < height:
                next_mid = density[planes - 1, r + 1, t] + some * plane[r + 1, t]
                below = jnp.where(row_end, pltpu.roll(next_mid, SUB - 1, 0), below)
            line.append(weights[0, r] * mid + weights[1, r] * below)
        turned = [pltpu.roll(m, LANES - 1, 1) for m in line]
        for t in range(tiles):
            beside = jnp.where(lane_end, turned[min(t + 1, tiles - 1)], turned[t])
            value.append(columns[0, t : t + 1, :] * line[t] + columns[1, t : t + 1, :] * beside)
    group = 4
    count = len(value)
    for first in range(0, count, group):
        absorption, emission = hats(value[first : first + group], table, levels)
        for j, (a, e) in enumerate(zip(absorption, emission, strict=True), first):
            i, t = divmod(j, tiles)
            through = before[1, i, t]
            behind = through * jnp.exp2(a * wide(masks[t : t + 1, :]))
            state[0, i, t] = before[0, i, t] + (through - behind) * e
            state[1, i, t] = behind


def upper_kernel(
    density, plane, row, table, masks, columns, weights, before, state, row_sums
):
    planes, height, tiles = density.shape[:3]
    for z in range(planes - 1):
        row_sums[z] = row[z] + row[z + 1]
    after = jnp.concatenate([plane[0, t, :1, :] for t in range(tiles)], 0)
    row_sums[planes - 1] = row[planes - 1] + unless_last("depth") * after
    add_last_plane(
        density, plane, table, masks, columns, weights, before, state, range(height - 1)
    )


def lower_kernel(
    density, plane, below, last_row, table, masks, columns, rows, weights, before, state
):
    planes, height, tiles = density.shape[:3]
    levels = table.shape[0] // 2
    add_last_plane(density, plane, table, masks, columns, weights, before, state, [height - 1])

    shape = (tiles, LANES)
    fold_end = lax.broadcasted_iota(jnp.int32, shape, 1) == LANES - 1
    near, far = rows[0:1, :], unless_last("rows") * rows[1:2, :]
    left, right = columns[0], columns[1]
    after = jnp.concatenate([plane[height - 1, t, SUB - 1 :, :] for t in range(tiles)], 0)
    own = [last_row[z] for z in range(planes)] + [unless_last("depth") * after]
    value = []
    for z in range(planes):
        line = near * (own[z] + own[z + 1]) + far * below[z]
        turned = pltpu.roll(line, LANES - 1, 1)
        beside = jnp.where(fold_end, pltpu.roll(turned, tiles - 1, 0), turned)
        value.append(left * line + right * beside)
    total = jnp.zeros(shape, F32)
    through = jnp.ones(shape, F32)
    light = jnp.zeros(shape, F32)
    group = 4
    for first in range(0, planes, group):
        absorption, emission = hats(value[first : first + group], table, levels)
        for a, e in zip(absorption, emission, strict=True):
            total = total + a * masks[...]
            behind = jnp.exp2(total)
            light = light + (through - behind) * e
            through = behind
    for t in range(tiles):
        state[0, 0, t, SUB - 1 :, :] = light[t : t + 1, :]
        state[1, 0, t, SUB - 1 :, :] = through[t : t + 1, :]


def is_behind(step):
    return (lax.axis_index("depth") & step) != 0


def merge(state, other, front, step):
    behind = is_behind(step)
    first = jnp.where(behind, other, state)
    second = jnp.where(behind, state, other)
    front = front * jnp.where(behind, other[1:], 1.0)
    return jnp.stack([first[0] + first[1] * second[0], first[1] * second[1]]), front


def last_merge_kernel(*refs, step, parts):
    ins, (front_out, image_out, front_buf, image_buf, sems) = refs[: 3 * parts], refs[3 * parts :]
    behind = is_behind(step)
    first, copies = 0, []
    for part in range(parts):
        state, other, front = ins[3 * part : 3 * part + 3]
        at = pl.ds(first, state.shape[1])
        first += state.shape[1]
        light, through = state[0], state[1]
        other_light, other_through = other[0], other[1]
        front_buf[0, at] = front[0] * jnp.where(behind, other_through, 1.0)
        image_buf[0, at] = jnp.where(
            behind, other_light + other_through * light, light + through * other_light
        )
        image_buf[1, at] = through * other_through
        copies += [
            pltpu.make_async_copy(front_buf.at[:, at], front_out.at[:, at], sems.at[2 * part]),
            pltpu.make_async_copy(image_buf.at[:, at], image_out.at[:, at], sems.at[2 * part + 1]),
        ]
        copies[-2].start()
        copies[-1].start()
    for copy in copies:
        copy.wait()


def on_device(density, bin_of_level, absorb_bins, emit_bins, occupancy, col_offsets, row_offsets):
    planes, rows, cols = density.shape
    height, tiles = rows // SUB, cols // LANES
    levels = bin_of_level.shape[0]
    tiled = density.reshape(planes, height, SUB, tiles, LANES).transpose(0, 1, 3, 2, 4)
    flat = (height, tiles, SUB, LANES)
    upper = (2, height - 1, tiles, SUB, LANES)
    lower = (2, 1, tiles, SUB, LANES)

    def out(*shape):
        return jax.ShapeDtypeStruct(shape, F32)

    small = (
        bin_of_level[None], absorb_bins[None], emit_bins[None], occupancy.reshape(1, tiles),
        row_offsets[None], col_offsets.reshape(tiles, LANES),
    )
    plane, row, last_row, *small = pl.pallas_call(
        edges_kernel,
        out_shape=[
            out(*flat), out(planes, tiles, LANES), out(planes, tiles, LANES),
            *[jax.ShapeDtypeStruct(x.shape, x.dtype) for x in small],
        ],
        in_specs=[HBM] * 7,
        out_specs=[VMEM] * 9,
        scratch_shapes=[pltpu.SemaphoreType.DMA((9,))],
        compiler_params=params(2),
        name="edges",
    )(*[pltpu.with_memory_space_constraint(x, pltpu.HBM) for x in (tiled, *small)])
    plane = plane_from_behind(plane)

    work = density.size
    above, under, table, masks, columns, last_weights, weights = pl.pallas_call(
        interior_kernel,
        out_shape=[
            out(*upper), out(*lower), out(2 * levels, LANES), out(tiles, LANES),
            out(2, tiles, LANES), out(2, LANES), out(2, height, SUB, LANES),
        ],
        in_specs=[VMEM] * 7,
        out_specs=[VMEM] * 7,
        scratch_shapes=[pltpu.VMEM((planes - 1, *flat), F32), pltpu.VMEM((SUB, LANES), F32)],
        cost_estimate=pl.CostEstimate(
            flops=100 * work, bytes_accessed=4 * work, transcendentals=work
        ),
        compiler_params=params(8),
        name="interior",
    )(*small, tiled)
    above, row = pl.pallas_call(
        upper_kernel,
        out_shape=[out(*upper), out(planes, tiles, LANES)],
        in_specs=[VMEM] * 8,
        out_specs=[VMEM] * 2,
        compiler_params=params(8),
        name="upper",
    )(tiled, plane, row, table, masks, columns, weights, above)
    row = from_behind(row, "rows")
    under = pl.pallas_call(
        lower_kernel,
        out_shape=out(*lower),
        in_specs=[VMEM] * 10,
        out_specs=VMEM,
        cost_estimate=pl.CostEstimate(
            flops=10 * work, bytes_accessed=work, transcendentals=work // 8
        ),
        compiler_params=params(8),
        name="lower",
    )(tiled, plane, row, last_row, table, masks, columns, last_weights, weights, under)

    size = lax.axis_size("depth")
    states = [above, under]
    fronts = [jnp.ones((1, *part.shape[1:]), F32) for part in states]
    step = 1
    while 2 * step < size:
        route = [(i, i ^ step) for i in range(size)]
        others = [lax.ppermute(state, "depth", route) for state in states]
        merged = [
            merge(state, other, front, step)
            for state, other, front in zip(states, others, fronts, strict=True)
        ]
        states, fronts = zip(*merged, strict=True)
        step *= 2
    route = [(i, i ^ step) for i in range(size)]
    others = [lax.ppermute(state, "depth", route) for state in states]
    parts = len(states)
    front, image = pl.pallas_call(
        functools.partial(last_merge_kernel, step=step, parts=parts),
        out_shape=[out(1, *flat), out(2, *flat)],
        in_specs=[VMEM] * (3 * parts),
        out_specs=[HBM] * 2,
        scratch_shapes=[
            pltpu.VMEM((1, *flat), F32),
            pltpu.VMEM((2, *flat), F32),
            pltpu.SemaphoreType.DMA((2 * parts,)),
        ],
        compiler_params=params(4),
        name="last_merge",
    )(*[ref for group in zip(states, others, fronts, strict=True) for ref in group])

    def plain(block):
        return block.transpose(0, 1, 3, 2, 4).reshape(-1, rows, cols)

    return (plain(front), plain(image))


def solution(mesh):
    placed = (P("depth", "rows", None), P(), P(), P(), P("depth", "rows", None), P(), P("rows"))
    return jax.shard_map(
        on_device,
        mesh=mesh,
        in_specs=placed,
        out_specs=(P("depth", "rows", None), P(None, "rows", None)),
        check_vma=False,
    )
```

```python
import functools
import math

import jax
import jax.numpy as jnp
from jax import lax
from jax.experimental import pallas as pl
from jax.experimental.pallas import tpu as pltpu
from jax.sharding import PartitionSpec as P

SUB, LANES = 8, 128
F32 = jnp.float32
VMEM = pl.BlockSpec(memory_space=pltpu.VMEM)
HBM = pl.BlockSpec(memory_space=pltpu.HBM)
SPAN = 5


def params(mib):
    return pltpu.CompilerParams(vmem_limit_bytes=mib << 20)


def from_behind(block, axis):
    size = lax.axis_size(axis)
    return lax.ppermute(block, axis, [((i + 1) % size, i) for i in range(size)])


def plane_from_behind(plane):
    depth, rows = lax.axis_size("depth"), lax.axis_size("rows")
    route = []
    for d in range(depth):
        for r in range(rows):
            end = d in (0, depth - 1)
            e, q = (d, r ^ 1) if end else ((d + 1 if d % 2 else d - 1), r)
            route.append((e * rows + q, d * rows + r))
    odd = lax.ppermute(plane, ("depth", "rows"), route)
    even = lax.ppermute(plane, "depth", [(i, i ^ 1) for i in range(depth)])
    return jnp.where(lax.axis_index("depth") % 2 == 0, even, odd)


def unless_last(axis):
    return jnp.where(lax.axis_index(axis) == lax.axis_size(axis) - 1, 0.0, 1.0)


def wide(row):
    return jnp.broadcast_to(row, (SUB, LANES))


def edges_kernel(density, *refs):
    small, (plane, *small_out), sems = refs[:6], refs[6:13], refs[13]
    pieces = [(density.at[0], plane), *zip(small, small_out, strict=True)]
    copies = [pltpu.make_async_copy(a, b, sems.at[i]) for i, (a, b) in enumerate(pieces)]
    for copy in copies:
        copy.start()
    for copy in copies:
        copy.wait()


def hats(values, table):
    pieces = table.shape[0] // (2 * (SPAN + 1))
    results = []
    for u in values:
        within = [u >= float(SPAN * i) for i in range(1, pieces)]

        def pick(rows, within=within):
            chosen = rows[0]
            for at, row in zip(within, rows[1:], strict=True):
                chosen = jnp.where(at, row, chosen)
            return chosen

        t = u - pick([jnp.full((SUB, LANES), float(SPAN * i), F32) for i in range(pieces)])
        kinks = [t] + [jnp.maximum(t, float(j)) for j in range(1, SPAN)]
        sums = []
        for which in range(2):

            def entry(q, which=which):
                first = which * pieces * (SPAN + 1) + q
                return pick(
                    [wide(table[k : k + 1, :]) for k in range(
                        first, first + pieces * (SPAN + 1), SPAN + 1)]
                )

            total = entry(0)
            for j, kink in enumerate(kinks):
                total = total + entry(j + 1) * kink
            sums.append(total)
        results.append(sums)
    return [r[0] for r in results], [r[1] for r in results]


def tables_kernel(
    bins, absorb_bins, emit_bins, occupied, row_offsets, col_offsets,
    table, masks, columns, rows, weights, small,
):
    height, tiles = weights.shape[1], masks.shape[0]
    levels = bins.shape[1]
    small[...] = jnp.zeros_like(small)
    for i, source in enumerate((bins, absorb_bins, emit_bins, occupied, row_offsets)):
        small[i : i + 1, : source.shape[1]] = source[...].astype(F32)
    fraction = col_offsets[...].astype(F32) * 0.125
    shape = fraction.shape
    ends = (lax.broadcasted_iota(jnp.int32, shape, 0) == tiles - 1) & (
        lax.broadcasted_iota(jnp.int32, shape, 1) == LANES - 1
    )
    columns[0] = 1.0 - fraction
    columns[1] = jnp.where(ends, 0.0, fraction)
    lane = lax.broadcasted_iota(jnp.int32, (SUB, LANES), 1)
    sub = lax.broadcasted_iota(jnp.int32, (SUB, LANES), 0)
    bins, absorb_bins, emit_bins, occupied, row_offsets = (
        wide(small[i : i + 1, :]) for i in range(5)
    )

    def pick(vector, k):
        return jnp.broadcast_to(vector[:, k : k + 1], (SUB, LANES))

    scale = 0.5 * (levels - 1)
    near, far = [], []
    for r in range(height):
        offset = jnp.zeros((SUB, LANES), F32)
        for i in range(SUB):
            offset = jnp.where(sub == i, pick(row_offsets, r * SUB + i), offset)
        far.append(offset * (scale / 8.0))
        near.append(scale - far[r])
        weights[0, r] = near[r]
        weights[1, r] = far[r]
    rows[0:1, :] = near[-1][SUB - 1 :, :]
    rows[1:2, :] = far[-1][SUB - 1 :, :]
    for t in range(tiles):
        masks[t : t + 1, :] = pick(occupied, t)[:1, :]

    which = bins.astype(jnp.int32)
    pieces = table.shape[0] // (2 * (SPAN + 1))
    row = 0
    for level, unit in ((absorb_bins, -1.0 / math.log(2.0)), (emit_bins, 1.0)):
        value = jnp.take_along_axis(level, which, axis=1, mode="promise_in_bounds") * unit
        slope = pltpu.roll(value, LANES - 1, 1) - value
        gain = slope - pltpu.roll(slope, 1, 1)
        base = value
        for j in range(1, SPAN):
            base = base - float(j) * pltpu.roll(gain, LANES - j, 1)
        for i in range(pieces):
            entries = [(base, 0), (slope, 0)] + [(gain, j) for j in range(1, SPAN)]
            for vector, j in entries:
                table[row : row + 1, :] = pick(vector, SPAN * i + j)[:1, :]
                row += 1


def interior_kernel(
    table, masks, columns, weights, density, state, last_state, row, last_row, scaled, sems
):
    planes, height, tiles = density.shape[:3]
    copies = [
        pltpu.make_async_copy(density.at[:, 0, :, 0, :], row, sems.at[0]),
        pltpu.make_async_copy(density.at[:, height - 1, :, SUB - 1, :], last_row, sems.at[1]),
    ]
    for copy in copies:
        copy.start()
    lane_end = lax.broadcasted_iota(jnp.int32, (SUB, LANES), 1) == LANES - 1
    row_end = lax.broadcasted_iota(jnp.int32, (SUB, LANES), 0) == SUB - 1
    near = [weights[0, r] for r in range(height)]
    far = [weights[1, r] for r in range(height)]

    for z in range(planes - 1):

        def mixed(t):
            mid = [density[z, r, t] + density[z + 1, r, t] for r in range(height)]
            up = [pltpu.roll(m, SUB - 1, 0) for m in mid]
            below = [
                jnp.where(row_end, up[r + 1], up[r]) if r + 1 < height else up[r]
                for r in range(height)
            ]
            return [near[r] * mid[r] + far[r] * below[r] for r in range(height)]

        now = mixed(0)
        turned = [pltpu.roll(m, LANES - 1, 1) for m in now]
        for t in range(tiles):
            if t + 1 < tiles:
                after = mixed(t + 1)
                after_turned = [pltpu.roll(m, LANES - 1, 1) for m in after]
            else:
                after, after_turned = now, turned
            left, right = columns[0, t : t + 1, :], columns[1, t : t + 1, :]
            for r in range(height):
                beside = jnp.where(lane_end, after_turned[r], turned[r])
                scaled[z, r, t] = left * now[r] + right * beside
            now, turned = after, after_turned

    @pl.loop(0, tiles)
    def _(t):
        mask = wide(masks[pl.ds(t, 1), :])
        total = [jnp.zeros((SUB, LANES), F32)] * height
        through = [jnp.ones((SUB, LANES), F32)] * height
        light = [jnp.zeros((SUB, LANES), F32)] * height
        for z in range(planes - 1):
            absorption, emission = hats([scaled[z, r, t] for r in range(height)], table)
            for r in range(height):
                total[r] = total[r] + absorption[r] * mask
                behind = jnp.exp2(total[r])
                light[r] = light[r] + (through[r] - behind) * emission[r]
                through[r] = behind
        for r in range(height - 1):
            state[0, r, t] = light[r]
            state[1, r, t] = through[r]
        last_state[0, 0, t] = light[-1]
        last_state[1, 0, t] = through[-1]

    for copy in copies:
        copy.wait()


def add_last_plane(density, plane, table, masks, columns, weights, before, state, tiles_of_rows):
    planes, height, tiles = density.shape[:3]
    some = unless_last("depth")
    lane_end = lax.broadcasted_iota(jnp.int32, (SUB, LANES), 1) == LANES - 1
    row_end = lax.broadcasted_iota(jnp.int32, (SUB, LANES), 0) == SUB - 1
    value = []
    for r in tiles_of_rows:
        line = []
        for t in range(tiles):
            mid = density[planes - 1, r, t] + some * plane[r, t]
            below = pltpu.roll(mid, SUB - 1, 0)
            if r + 1 < height:
                next_mid = density[planes - 1, r + 1, t] + some * plane[r + 1, t]
                below = jnp.where(row_end, pltpu.roll(next_mid, SUB - 1, 0), below)
            line.append(weights[0, r] * mid + weights[1, r] * below)
        turned = [pltpu.roll(m, LANES - 1, 1) for m in line]
        for t in range(tiles):
            beside = jnp.where(lane_end, turned[min(t + 1, tiles - 1)], turned[t])
            value.append(columns[0, t : t + 1, :] * line[t] + columns[1, t : t + 1, :] * beside)
    group = 4
    count = len(value)
    for first in range(0, count, group):
        absorption, emission = hats(value[first : first + group], table)
        for j, (a, e) in enumerate(zip(absorption, emission, strict=True), first):
            i, t = divmod(j, tiles)
            through = before[1, i, t]
            behind = through * jnp.exp2(a * wide(masks[t : t + 1, :]))
            state[0, i, t] = before[0, i, t] + (through - behind) * e
            state[1, i, t] = behind


def upper_kernel(
    density, plane, row, table, masks, columns, weights, before, state, row_sums
):
    planes, height, tiles = density.shape[:3]
    for z in range(planes - 1):
        row_sums[z] = row[z] + row[z + 1]
    after = jnp.concatenate([plane[0, t, :1, :] for t in range(tiles)], 0)
    row_sums[planes - 1] = row[planes - 1] + unless_last("depth") * after
    add_last_plane(
        density, plane, table, masks, columns, weights, before, state, range(height - 1)
    )


def lower_kernel(
    density, plane, below, last_row, table, masks, columns, rows, weights, before, state
):
    planes, height, tiles = density.shape[:3]
    add_last_plane(density, plane, table, masks, columns, weights, before, state, [height - 1])

    shape = (tiles, LANES)
    fold_end = lax.broadcasted_iota(jnp.int32, shape, 1) == LANES - 1
    near, far = rows[0:1, :], unless_last("rows") * rows[1:2, :]
    left, right = columns[0], columns[1]
    after = jnp.concatenate([plane[height - 1, t, SUB - 1 :, :] for t in range(tiles)], 0)
    own = [last_row[z] for z in range(planes)] + [unless_last("depth") * after]
    value = []
    for z in range(planes):
        line = near * (own[z] + own[z + 1]) + far * below[z]
        turned = pltpu.roll(line, LANES - 1, 1)
        beside = jnp.where(fold_end, pltpu.roll(turned, tiles - 1, 0), turned)
        value.append(left * line + right * beside)
    total = jnp.zeros(shape, F32)
    through = jnp.ones(shape, F32)
    light = jnp.zeros(shape, F32)
    group = 4
    for first in range(0, planes, group):
        absorption, emission = hats(value[first : first + group], table)
        for a, e in zip(absorption, emission, strict=True):
            total = total + a * masks[...]
            behind = jnp.exp2(total)
            light = light + (through - behind) * e
            through = behind
    for t in range(tiles):
        state[0, 0, t, SUB - 1 :, :] = light[t : t + 1, :]
        state[1, 0, t, SUB - 1 :, :] = through[t : t + 1, :]


def is_behind(step):
    return (lax.axis_index("depth") & step) != 0


def merge(state, other, front, step):
    behind = is_behind(step)
    first = jnp.where(behind, other, state)
    second = jnp.where(behind, state, other)
    front = front * jnp.where(behind, other[1:], 1.0)
    return jnp.stack([first[0] + first[1] * second[0], first[1] * second[1]]), front


def last_merge_kernel(*refs, step, parts):
    ins, (front_out, image_out, front_buf, image_buf, sems) = refs[: 3 * parts], refs[3 * parts :]
    behind = is_behind(step)
    first, copies = 0, []
    for part in range(parts):
        state, other, front = ins[3 * part : 3 * part + 3]
        at = pl.ds(first, state.shape[1])
        first += state.shape[1]
        light, through = state[0], state[1]
        other_light, other_through = other[0], other[1]
        front_buf[0, at] = front[0] * jnp.where(behind, other_through, 1.0)
        image_buf[0, at] = jnp.where(
            behind, other_light + other_through * light, light + through * other_light
        )
        image_buf[1, at] = through * other_through
        copies += [
            pltpu.make_async_copy(front_buf.at[:, at], front_out.at[:, at], sems.at[2 * part]),
            pltpu.make_async_copy(image_buf.at[:, at], image_out.at[:, at], sems.at[2 * part + 1]),
        ]
        copies[-2].start()
        copies[-1].start()
    for copy in copies:
        copy.wait()


def on_device(density, bin_of_level, absorb_bins, emit_bins, occupancy, col_offsets, row_offsets):
    planes, rows, cols = density.shape
    height, tiles = rows // SUB, cols // LANES
    pieces = -(-(bin_of_level.shape[0] - 1) // SPAN)
    tiled = density.reshape(planes, height, SUB, tiles, LANES).transpose(0, 1, 3, 2, 4)
    flat = (height, tiles, SUB, LANES)
    upper = (2, height - 1, tiles, SUB, LANES)
    lower = (2, 1, tiles, SUB, LANES)

    def out(*shape):
        return jax.ShapeDtypeStruct(shape, F32)

    small = (
        bin_of_level[None], absorb_bins[None], emit_bins[None], occupancy.reshape(1, tiles),
        row_offsets[None], col_offsets.reshape(tiles, LANES),
    )
    plane, *small = pl.pallas_call(
        edges_kernel,
        out_shape=[
            out(*flat),
            *[jax.ShapeDtypeStruct(x.shape, x.dtype) for x in small],
        ],
        in_specs=[HBM] * 7,
        out_specs=[VMEM] * 7,
        scratch_shapes=[pltpu.SemaphoreType.DMA((7,))],
        compiler_params=params(2),
        name="edges",
    )(*[pltpu.with_memory_space_constraint(x, pltpu.HBM) for x in (tiled, *small)])
    plane = plane_from_behind(plane)

    work = density.size
    table, masks, columns, last_weights, weights = pl.pallas_call(
        tables_kernel,
        out_shape=[
            out(2 * (SPAN + 1) * pieces, LANES), out(tiles, LANES), out(2, tiles, LANES), out(2, LANES),
            out(2, height, SUB, LANES),
        ],
        in_specs=[VMEM] * 6,
        out_specs=[VMEM] * 5,
        scratch_shapes=[pltpu.VMEM((SUB, LANES), F32)],
        compiler_params=params(1),
        name="tables",
    )(*small)
    above, under, row, last_row = pl.pallas_call(
        interior_kernel,
        out_shape=[
            out(*upper), out(*lower), out(planes, tiles, LANES), out(planes, tiles, LANES)
        ],
        in_specs=[VMEM] * 5,
        out_specs=[VMEM] * 4,
        scratch_shapes=[pltpu.VMEM((planes - 1, *flat), F32), pltpu.SemaphoreType.DMA((2,))],
        cost_estimate=pl.CostEstimate(
            flops=100 * work, bytes_accessed=4 * work, transcendentals=work
        ),
        compiler_params=params(8),
        name="interior",
    )(table, masks, columns, weights, tiled)
    above, row = pl.pallas_call(
        upper_kernel,
        out_shape=[out(*upper), out(planes, tiles, LANES)],
        in_specs=[VMEM] * 8,
        out_specs=[VMEM] * 2,
        compiler_params=params(8),
        name="upper",
    )(tiled, plane, row, table, masks, columns, weights, above)
    row = from_behind(row, "rows")
    under = pl.pallas_call(
        lower_kernel,
        out_shape=out(*lower),
        in_specs=[VMEM] * 10,
        out_specs=VMEM,
        cost_estimate=pl.CostEstimate(
            flops=10 * work, bytes_accessed=work, transcendentals=work // 8
        ),
        compiler_params=params(8),
        name="lower",
    )(tiled, plane, row, last_row, table, masks, columns, last_weights, weights, under)

    size = lax.axis_size("depth")
    states = [above, under]
    fronts = [jnp.ones((1, *part.shape[1:]), F32) for part in states]
    step = 1
    while 2 * step < size:
        route = [(i, i ^ step) for i in range(size)]
        others = [lax.ppermute(state, "depth", route) for state in states]
        merged = [
            merge(state, other, front, step)
            for state, other, front in zip(states, others, fronts, strict=True)
        ]
        states, fronts = zip(*merged, strict=True)
        step *= 2
    route = [(i, i ^ step) for i in range(size)]
    others = [lax.ppermute(state, "depth", route) for state in states]
    parts = len(states)
    front, image = pl.pallas_call(
        functools.partial(last_merge_kernel, step=step, parts=parts),
        out_shape=[out(1, *flat), out(2, *flat)],
        in_specs=[VMEM] * (3 * parts),
        out_specs=[HBM] * 2,
        scratch_shapes=[
            pltpu.VMEM((1, *flat), F32),
            pltpu.VMEM((2, *flat), F32),
            pltpu.SemaphoreType.DMA((2 * parts,)),
        ],
        compiler_params=params(4),
        name="last_merge",
    )(*[ref for group in zip(states, others, fronts, strict=True) for ref in group])

    def plain(block):
        return block.transpose(0, 1, 3, 2, 4).reshape(-1, rows, cols)

    return (plain(front), plain(image))


def solution(mesh):
    placed = (P("depth", "rows", None), P(), P(), P(), P("depth", "rows", None), P(), P("rows"))
    return jax.shard_map(
        on_device,
        mesh=mesh,
        in_specs=placed,
        out_specs=(P("depth", "rows", None), P(None, "rows", None)),
        check_vma=False,
    )
```

```python
import functools
import math

import jax
import jax.numpy as jnp
from jax import lax
from jax.experimental import pallas as pl
from jax.experimental.pallas import tpu as pltpu
from jax.sharding import PartitionSpec as P

SUB, LANES = 8, 128
F32 = jnp.float32
VMEM = pl.BlockSpec(memory_space=pltpu.VMEM)
HBM = pl.BlockSpec(memory_space=pltpu.HBM)
SPAN = 5


def params(mib):
    return pltpu.CompilerParams(vmem_limit_bytes=mib << 20)


def from_behind(block, axis):
    size = lax.axis_size(axis)
    return lax.ppermute(block, axis, [((i + 1) % size, i) for i in range(size)])


def plane_from_behind(plane):
    depth, rows = lax.axis_size("depth"), lax.axis_size("rows")
    route = []
    for d in range(depth):
        for r in range(rows):
            end = d in (0, depth - 1)
            e, q = (d, r ^ 1) if end else ((d + 1 if d % 2 else d - 1), r)
            route.append((e * rows + q, d * rows + r))
    odd = lax.ppermute(plane, ("depth", "rows"), route)
    even = lax.ppermute(plane, "depth", [(i, i ^ 1) for i in range(depth)])
    return jnp.where(lax.axis_index("depth") % 2 == 0, even, odd)


def unless_last(axis):
    return jnp.where(lax.axis_index(axis) == lax.axis_size(axis) - 1, 0.0, 1.0)


def wide(row):
    return jnp.broadcast_to(row, (SUB, LANES))


def edges_kernel(density, *refs):
    small, (plane, *small_out), sems = refs[:6], refs[6:13], refs[13]
    pieces = [(density.at[0], plane), *zip(small, small_out, strict=True)]
    copies = [pltpu.make_async_copy(a, b, sems.at[i]) for i, (a, b) in enumerate(pieces)]
    for copy in copies:
        copy.start()
    for copy in copies:
        copy.wait()


def hats(values, table):
    pieces = table.shape[0] // (2 * (SPAN + 1))
    results = []
    for u in values:
        within = [u >= float(SPAN * i) for i in range(1, pieces)]

        def pick(rows, within=within):
            chosen = rows[0]
            for at, row in zip(within, rows[1:], strict=True):
                chosen = jnp.where(at, row, chosen)
            return chosen

        t = u - pick([jnp.full((SUB, LANES), float(SPAN * i), F32) for i in range(pieces)])
        kinks = [t] + [jnp.maximum(t, float(j)) for j in range(1, SPAN)]
        sums = []
        for which in range(2):

            def entry(q, which=which):
                first = which * pieces * (SPAN + 1) + q
                return pick(
                    [wide(table[k : k + 1, :]) for k in range(
                        first, first + pieces * (SPAN + 1), SPAN + 1)]
                )

            total = entry(0)
            for j, kink in enumerate(kinks):
                total = total + entry(j + 1) * kink
            sums.append(total)
        results.append(sums)
    return [r[0] for r in results], [r[1] for r in results]


def tables_kernel(
    bins, absorb_bins, emit_bins, occupied, row_offsets, col_offsets,
    table, masks, columns, rows, weights, small,
):
    height, tiles = weights.shape[1], masks.shape[0]
    levels = bins.shape[1]
    small[...] = jnp.zeros_like(small)
    for i, source in enumerate((bins, absorb_bins, emit_bins, occupied, row_offsets)):
        small[i : i + 1, : source.shape[1]] = source[...].astype(F32)
    fraction = col_offsets[...].astype(F32) * 0.125
    shape = fraction.shape
    ends = (lax.broadcasted_iota(jnp.int32, shape, 0) == tiles - 1) & (
        lax.broadcasted_iota(jnp.int32, shape, 1) == LANES - 1
    )
    columns[0] = 1.0 - fraction
    columns[1] = jnp.where(ends, 0.0, fraction)
    lane = lax.broadcasted_iota(jnp.int32, (SUB, LANES), 1)
    sub = lax.broadcasted_iota(jnp.int32, (SUB, LANES), 0)
    bins, absorb_bins, emit_bins, occupied, row_offsets = (
        wide(small[i : i + 1, :]) for i in range(5)
    )

    def pick(vector, k):
        return jnp.broadcast_to(vector[:, k : k + 1], (SUB, LANES))

    scale = 0.5 * (levels - 1)
    near, far = [], []
    for r in range(height):
        offset = jnp.zeros((SUB, LANES), F32)
        for i in range(SUB):
            offset = jnp.where(sub == i, pick(row_offsets, r * SUB + i), offset)
        far.append(offset * (scale / 8.0))
        near.append(scale - far[r])
        weights[0, r] = near[r]
        weights[1, r] = far[r]
    rows[0:1, :] = near[-1][SUB - 1 :, :]
    rows[1:2, :] = far[-1][SUB - 1 :, :]
    for t in range(tiles):
        masks[t : t + 1, :] = pick(occupied, t)[:1, :]

    which = bins.astype(jnp.int32)
    pieces = table.shape[0] // (2 * (SPAN + 1))
    row = 0
    for level, unit in ((absorb_bins, -1.0 / math.log(2.0)), (emit_bins, 1.0)):
        value = jnp.take_along_axis(level, which, axis=1, mode="promise_in_bounds") * unit
        slope = pltpu.roll(value, LANES - 1, 1) - value
        gain = slope - pltpu.roll(slope, 1, 1)
        base = value
        for j in range(1, SPAN):
            base = base - float(j) * pltpu.roll(gain, LANES - j, 1)
        for i in range(pieces):
            entries = [(base, 0), (slope, 0)] + [(gain, j) for j in range(1, SPAN)]
            for vector, j in entries:
                table[row : row + 1, :] = pick(vector, SPAN * i + j)[:1, :]
                row += 1


def interior_kernel(
    table, masks, columns, weights, density, state, last_state, row, last_row, scaled, sems
):
    planes, height, tiles = density.shape[:3]
    copies = [
        pltpu.make_async_copy(density.at[:, 0, :, 0, :], row, sems.at[0]),
        pltpu.make_async_copy(density.at[:, height - 1, :, SUB - 1, :], last_row, sems.at[1]),
    ]
    for copy in copies:
        copy.start()
    lane_end = lax.broadcasted_iota(jnp.int32, (SUB, LANES), 1) == LANES - 1
    row_end = lax.broadcasted_iota(jnp.int32, (SUB, LANES), 0) == SUB - 1
    near = [weights[0, r] for r in range(height)]
    far = [weights[1, r] for r in range(height)]

    for z in range(planes - 1):

        def mixed(t):
            mid = [density[z, r, t] + density[z + 1, r, t] for r in range(height)]
            up = [pltpu.roll(m, SUB - 1, 0) for m in mid]
            below = [
                jnp.where(row_end, up[r + 1], up[r]) if r + 1 < height else up[r]
                for r in range(height)
            ]
            return [near[r] * mid[r] + far[r] * below[r] for r in range(height)]

        now = mixed(0)
        turned = [pltpu.roll(m, LANES - 1, 1) for m in now]
        for t in range(tiles):
            if t + 1 < tiles:
                after = mixed(t + 1)
                after_turned = [pltpu.roll(m, LANES - 1, 1) for m in after]
            else:
                after, after_turned = now, turned
            left, right = columns[0, t : t + 1, :], columns[1, t : t + 1, :]
            for r in range(height):
                beside = jnp.where(lane_end, after_turned[r], turned[r])
                scaled[z, r, t] = left * now[r] + right * beside
            now, turned = after, after_turned

    @pl.loop(0, tiles)
    def _(t):
        mask = wide(masks[pl.ds(t, 1), :])
        total = [jnp.zeros((SUB, LANES), F32)] * height
        through = [jnp.ones((SUB, LANES), F32)] * height
        light = [jnp.zeros((SUB, LANES), F32)] * height
        for z in range(planes - 1):
            absorption, emission = hats([scaled[z, r, t] for r in range(height)], table)
            for r in range(height):
                total[r] = total[r] + absorption[r] * mask
                behind = jnp.exp2(total[r])
                light[r] = light[r] + (through[r] - behind) * emission[r]
                through[r] = behind
        for r in range(height - 1):
            state[0, r, t] = light[r]
            state[1, r, t] = through[r]
        last_state[0, 0, t] = light[-1]
        last_state[1, 0, t] = through[-1]

    for copy in copies:
        copy.wait()


def add_last_plane(density, plane, table, masks, columns, weights, before, state, tiles_of_rows):
    planes, height, tiles = density.shape[:3]
    some = unless_last("depth")
    lane_end = lax.broadcasted_iota(jnp.int32, (SUB, LANES), 1) == LANES - 1
    row_end = lax.broadcasted_iota(jnp.int32, (SUB, LANES), 0) == SUB - 1
    value = []
    for r in tiles_of_rows:
        line = []
        for t in range(tiles):
            mid = density[planes - 1, r, t] + some * plane[r, t]
            below = pltpu.roll(mid, SUB - 1, 0)
            if r + 1 < height:
                next_mid = density[planes - 1, r + 1, t] + some * plane[r + 1, t]
                below = jnp.where(row_end, pltpu.roll(next_mid, SUB - 1, 0), below)
            line.append(weights[0, r] * mid + weights[1, r] * below)
        turned = [pltpu.roll(m, LANES - 1, 1) for m in line]
        for t in range(tiles):
            beside = jnp.where(lane_end, turned[min(t + 1, tiles - 1)], turned[t])
            value.append(columns[0, t : t + 1, :] * line[t] + columns[1, t : t + 1, :] * beside)
    group = 4
    count = len(value)
    for first in range(0, count, group):
        absorption, emission = hats(value[first : first + group], table)
        for j, (a, e) in enumerate(zip(absorption, emission, strict=True), first):
            i, t = divmod(j, tiles)
            through = before[1, i, t]
            behind = through * jnp.exp2(a * wide(masks[t : t + 1, :]))
            state[0, i, t] = before[0, i, t] + (through - behind) * e
            state[1, i, t] = behind


def row_sums_kernel(plane, row, row_sums):
    planes, tiles = row.shape[:2]
    for z in range(planes - 1):
        row_sums[z] = row[z] + row[z + 1]
    after = jnp.concatenate([plane[0, t, :1, :] for t in range(tiles)], 0)
    row_sums[planes - 1] = row[planes - 1] + unless_last("depth") * after


def last_plane_kernel(
    density, plane, table, masks, columns, weights, above, under, above_out, under_out
):
    height = density.shape[1]
    args = (density, plane, table, masks, columns, weights)
    add_last_plane(*args, above, above_out, range(height - 1))
    add_last_plane(*args, under, under_out, [height - 1])


def last_row_kernel(plane, below, last_row, table, masks, columns, rows, before, state):
    height, tiles = plane.shape[:2]
    planes = below.shape[0]
    state[...] = before[...]
    shape = (tiles, LANES)
    fold_end = lax.broadcasted_iota(jnp.int32, shape, 1) == LANES - 1
    near, far = rows[0:1, :], unless_last("rows") * rows[1:2, :]
    left, right = columns[0], columns[1]
    after = jnp.concatenate([plane[height - 1, t, SUB - 1 :, :] for t in range(tiles)], 0)
    own = [last_row[z] for z in range(planes)] + [unless_last("depth") * after]
    value = []
    for z in range(planes):
        line = near * (own[z] + own[z + 1]) + far * below[z]
        turned = pltpu.roll(line, LANES - 1, 1)
        beside = jnp.where(fold_end, pltpu.roll(turned, tiles - 1, 0), turned)
        value.append(left * line + right * beside)
    total = jnp.zeros(shape, F32)
    through = jnp.ones(shape, F32)
    light = jnp.zeros(shape, F32)
    group = 4
    for first in range(0, planes, group):
        absorption, emission = hats(value[first : first + group], table)
        for a, e in zip(absorption, emission, strict=True):
            total = total + a * masks[...]
            behind = jnp.exp2(total)
            light = light + (through - behind) * e
            through = behind
    for t in range(tiles):
        state[0, 0, t, SUB - 1 :, :] = light[t : t + 1, :]
        state[1, 0, t, SUB - 1 :, :] = through[t : t + 1, :]


def is_behind(step):
    return (lax.axis_index("depth") & step) != 0


def merge(state, other, front, step):
    behind = is_behind(step)
    first = jnp.where(behind, other, state)
    second = jnp.where(behind, state, other)
    front = front * jnp.where(behind, other[1:], 1.0)
    return jnp.stack([first[0] + first[1] * second[0], first[1] * second[1]]), front


def last_merge_kernel(*refs, step, parts):
    ins, (front_out, image_out, front_buf, image_buf, sems) = refs[: 3 * parts], refs[3 * parts :]
    behind = is_behind(step)
    first, copies = 0, []
    for part in range(parts):
        state, other, front = ins[3 * part : 3 * part + 3]
        at = pl.ds(first, state.shape[1])
        first += state.shape[1]
        light, through = state[0], state[1]
        other_light, other_through = other[0], other[1]
        front_buf[0, at] = front[0] * jnp.where(behind, other_through, 1.0)
        image_buf[0, at] = jnp.where(
            behind, other_light + other_through * light, light + through * other_light
        )
        image_buf[1, at] = through * other_through
        copies += [
            pltpu.make_async_copy(front_buf.at[:, at], front_out.at[:, at], sems.at[2 * part]),
            pltpu.make_async_copy(image_buf.at[:, at], image_out.at[:, at], sems.at[2 * part + 1]),
        ]
        copies[-2].start()
        copies[-1].start()
    for copy in copies:
        copy.wait()


def on_device(density, bin_of_level, absorb_bins, emit_bins, occupancy, col_offsets, row_offsets):
    planes, rows, cols = density.shape
    height, tiles = rows // SUB, cols // LANES
    pieces = -(-(bin_of_level.shape[0] - 1) // SPAN)
    tiled = density.reshape(planes, height, SUB, tiles, LANES).transpose(0, 1, 3, 2, 4)
    flat = (height, tiles, SUB, LANES)
    upper = (2, height - 1, tiles, SUB, LANES)
    lower = (2, 1, tiles, SUB, LANES)

    def out(*shape):
        return jax.ShapeDtypeStruct(shape, F32)

    small = (
        bin_of_level[None], absorb_bins[None], emit_bins[None], occupancy.reshape(1, tiles),
        row_offsets[None], col_offsets.reshape(tiles, LANES),
    )
    plane, *small = pl.pallas_call(
        edges_kernel,
        out_shape=[
            out(*flat),
            *[jax.ShapeDtypeStruct(x.shape, x.dtype) for x in small],
        ],
        in_specs=[HBM] * 7,
        out_specs=[VMEM] * 7,
        scratch_shapes=[pltpu.SemaphoreType.DMA((7,))],
        compiler_params=params(2),
        name="edges",
    )(*[pltpu.with_memory_space_constraint(x, pltpu.HBM) for x in (tiled, *small)])
    plane = plane_from_behind(plane)

    work = density.size
    table, masks, columns, last_weights, weights = pl.pallas_call(
        tables_kernel,
        out_shape=[
            out(2 * (SPAN + 1) * pieces, LANES), out(tiles, LANES), out(2, tiles, LANES), out(2, LANES),
            out(2, height, SUB, LANES),
        ],
        in_specs=[VMEM] * 6,
        out_specs=[VMEM] * 5,
        scratch_shapes=[pltpu.VMEM((SUB, LANES), F32)],
        compiler_params=params(1),
        name="tables",
    )(*small)
    above, under, row, last_row = pl.pallas_call(
        interior_kernel,
        out_shape=[
            out(*upper), out(*lower), out(planes, tiles, LANES), out(planes, tiles, LANES)
        ],
        in_specs=[VMEM] * 5,
        out_specs=[VMEM] * 4,
        scratch_shapes=[pltpu.VMEM((planes - 1, *flat), F32), pltpu.SemaphoreType.DMA((2,))],
        cost_estimate=pl.CostEstimate(
            flops=100 * work, bytes_accessed=4 * work, transcendentals=work
        ),
        compiler_params=params(8),
        name="interior",
    )(table, masks, columns, weights, tiled)
    row = pl.pallas_call(
        row_sums_kernel,
        out_shape=out(planes, tiles, LANES),
        in_specs=[VMEM] * 2,
        out_specs=VMEM,
        compiler_params=params(1),
        name="row_sums",
    )(plane, row)
    row = from_behind(row, "rows")
    above, under = pl.pallas_call(
        last_plane_kernel,
        out_shape=[out(*upper), out(*lower)],
        in_specs=[VMEM] * 8,
        out_specs=[VMEM] * 2,
        cost_estimate=pl.CostEstimate(
            flops=10 * work, bytes_accessed=work, transcendentals=work // 8
        ),
        compiler_params=params(8),
        name="last_plane",
    )(tiled, plane, table, masks, columns, weights, above, under)
    under = pl.pallas_call(
        last_row_kernel,
        out_shape=out(*lower),
        in_specs=[VMEM] * 8,
        out_specs=VMEM,
        cost_estimate=pl.CostEstimate(
            flops=10 * work, bytes_accessed=work, transcendentals=work // 8
        ),
        compiler_params=params(8),
        name="last_row",
    )(plane, row, last_row, table, masks, columns, last_weights, under)

    size = lax.axis_size("depth")
    states = [above, under]
    fronts = [jnp.ones((1, *part.shape[1:]), F32) for part in states]
    step = 1
    while 2 * step < size:
        route = [(i, i ^ step) for i in range(size)]
        others = [lax.ppermute(state, "depth", route) for state in states]
        merged = [
            merge(state, other, front, step)
            for state, other, front in zip(states, others, fronts, strict=True)
        ]
        states, fronts = zip(*merged, strict=True)
        step *= 2
    route = [(i, i ^ step) for i in range(size)]
    others = [lax.ppermute(state, "depth", route) for state in states]
    parts = len(states)
    front, image = pl.pallas_call(
        functools.partial(last_merge_kernel, step=step, parts=parts),
        out_shape=[out(1, *flat), out(2, *flat)],
        in_specs=[VMEM] * (3 * parts),
        out_specs=[HBM] * 2,
        scratch_shapes=[
            pltpu.VMEM((1, *flat), F32),
            pltpu.VMEM((2, *flat), F32),
            pltpu.SemaphoreType.DMA((2 * parts,)),
        ],
        compiler_params=params(4),
        name="last_merge",
    )(*[ref for group in zip(states, others, fronts, strict=True) for ref in group])

    def plain(block):
        return block.transpose(0, 1, 3, 2, 4).reshape(-1, rows, cols)

    return (plain(front), plain(image))


def solution(mesh):
    placed = (P("depth", "rows", None), P(), P(), P(), P("depth", "rows", None), P(), P("rows"))
    return jax.shard_map(
        on_device,
        mesh=mesh,
        in_specs=placed,
        out_specs=(P("depth", "rows", None), P(None, "rows", None)),
        check_vma=False,
    )
```
